32 devices in a mesh: hst: 4 (over y, core), dev: 8 (over z, x).
Axes of the slice: x: 2, y: 2, z: 4, core: 2. Of those that a mesh axis runs over, the one named last changes fastest.
Arguments:
- hot_rows: bfloat16 [4096, 768], replicated, may hold values from -6 to 6
- cold_rows: bfloat16 [32768, 768], P(('hst', 'dev')), may hold values from -6 to 6
- hot_mask: int32 [65536], P(('hst', 'dev')), may hold values from 0 to 1, as said below
- hot_id: int32 [65536], P(('hst', 'dev')), may hold values from 0 to 4095
- cold_owner: int32 [65536], P(('hst', 'dev')), may hold values from 0 to 31, as said below
- cold_pos: int32 [65536], P(('hst', 'dev')), may hold values from 0 to 63, as said below
- cold_send: int32 [32, 2048], P(('hst', 'dev')), may hold values from 0 to 1023
- adjacency_one: int32 [65536, 15], P(('hst', 'dev')), may hold values from 0 to 2047
- adjacency_two: int32 [16384, 15], P(('hst', 'dev')), may hold values from 0 to 2303
- halo_send: int32 [32, 256], P(('hst', 'dev')), may hold values from 0 to 2047
- self_first: bfloat16 [768, 1024], replicated, may hold values from -0.21875 to 0.21875
- neigh_first: bfloat16 [768, 1024], replicated, may hold values from -0.21875 to 0.21875
- bn_gain: float32 [1024], replicated, may hold values from 0.1 to 1.9
- bn_shift: float32 [1024], replicated, may hold values from -3 to 3
- self_second: bfloat16 [1024, 153], replicated, may hold values from -0.1875 to 0.1875
- neigh_second: bfloat16 [1024, 153], replicated, may hold values from -0.1875 to 0.1875
Outputs:
- logits: float32 [16384, 153], P(('hst', 'dev'))
The draws below stay inside these ranges and needn't reach their ends.
Inputs may be any that keep to these rules, and one draw needn't show every extreme that they name: Each device has exactly 1536 nodes with hot_mask 0. `cold_owner`: for each device and owner, at most 64 of the device's nodes with hot_mask 0 name that owner; some owner is named by exactly 64 of them on every device. `cold_pos`: the nodes of one device with hot_mask 0 and the same owner have distinct slots.
All inputs are finite; a program needn't handle non-finite values.
Results may differ from the reference program's by a relative error of at most 0.003.
The reference program's roundings to bfloat16 on the way (of `features`, `first_mean`, `hidden`, `table` and `second_mean`) count: a program that leaves them out, or rounds other values in their place, can miss the bound.
Values may be sent and summed in bfloat16 or wider, within the bound.
A program may use at most 128 MiB of HBM per device.

```python
import math
import jax
import jax.numpy as jnp
import numpy as np
from jax import lax

F = 768
H = 1024
C = 153
L_DEV = 2048
COLD_DEV = 1024
HCAP = 32
HOT = 4096
K1 = 15
K2 = 15
COLD_NODES = 1536
B_DEV = 512
CAP = 64
NODES = 65536
TARGETS = 16384
COLD_ROWS = 32768
N_HST = 4
N_DEV = 8
DEVICES = 32


def cold_layout(key):
    base = jax.random.fold_in(key, 7)
    key_slots, key_nodes = jax.random.split(base)
    total_slots = DEVICES * CAP
    slot_index = jnp.arange(total_slots, dtype=jnp.int32)
    noise = jax.random.randint(key_slots, (DEVICES, total_slots), 0, 2 ** 19, dtype=jnp.int32)
    scores = noise * total_slots + slot_index[None, :]
    forced = (slot_index // CAP)[None, :] == ((jnp.arange(DEVICES, dtype=jnp.int32) + 1) % DEVICES)[:, None]
    scores = jnp.where(forced, slot_index[None, :] - total_slots, scores)
    chosen = jnp.argsort(scores, axis=1)[:, :COLD_NODES].astype(jnp.int32)
    owners = chosen // CAP
    positions = chosen % CAP
    node_noise = jax.random.randint(key_nodes, (DEVICES, L_DEV), 0, 2 ** 19, dtype=jnp.int32)
    node_scores = node_noise * L_DEV + jnp.arange(L_DEV, dtype=jnp.int32)[None, :]
    order = jnp.argsort(node_scores, axis=1)[:, :COLD_NODES].astype(jnp.int32)
    device_rows = jnp.broadcast_to(jnp.arange(DEVICES, dtype=jnp.int32)[:, None], order.shape)
    owner_full = jnp.zeros((DEVICES, L_DEV), jnp.int32).at[device_rows, order].set(owners)
    pos_full = jnp.zeros((DEVICES, L_DEV), jnp.int32).at[device_rows, order].set(positions)
    cold_flag = jnp.zeros((DEVICES, L_DEV), jnp.int32).at[device_rows, order].set(1)
    return (owner_full.reshape(-1), pos_full.reshape(-1), (1 - cold_flag).reshape(-1))


def draw_hot_mask(key, part):
    return cold_layout(key)[2]


def draw_cold_owner(key, part):
    return cold_layout(key)[0]


def draw_cold_pos(key, part):
    return cold_layout(key)[1]


def with_ends(drawn, rng, low, top_value):
    dims = drawn.shape
    place = [jax.random.randint(jax.random.fold_in(rng, axis), (), 0, dims[axis]) for axis in range(len(dims))]
    drawn = drawn.at[tuple(place)].set(low)
    longest = dims.index(max(dims))
    place[longest] = (place[longest] + 1) % dims[longest]
    return drawn.at[tuple(place)].set(top_value)


def shard_levels(rng, extent, pieces, low, high):
    level, own = 1.0, jax.random.fold_in(rng, 6)
    for dim, parts in pieces:
        draws = jnp.exp(jax.random.uniform(jax.random.fold_in(own, dim), (parts,), jnp.float32, low / len(pieces), high / len(pieces)))
        level = level * jnp.repeat(draws, extent[dim] // parts).reshape([-1 if axis == dim else 1 for axis in range(len(extent))])
    return level


def rank_table(count, slope):
    weights = [(1 << 20) // math.isqrt(standing ** slope) + 1 for standing in range(1, count + 1)]
    width = 1 + sum(weights) // (1 << 30)
    return np.cumsum(np.array([max(1, weight // width) for weight in weights]))


def ranked(own_key, dims, amount, skew):
    listing = rank_table(amount, skew)
    pick = jax.random.randint(jax.random.fold_in(own_key, 1), dims, 0, int(listing[amount - 1]))
    rank = jnp.searchsorted(jnp.asarray(listing, jnp.int32), pick, side="right")
    return jax.random.permutation(jax.random.fold_in(own_key, 2), amount)[rank].astype(jnp.int32)


def gaussian(rng, dims, deviation, bound, shards=(), kind=jnp.bfloat16):
    level = shard_levels(rng, dims, shards, -0.22, 0.18) if shards else 1.0
    values = jax.random.normal(rng, dims, jnp.float32) * deviation * level
    return jnp.minimum(jnp.maximum(values, -bound), bound).astype(kind)


def setup_inputs(seed: int = 0) -> dict:
    arg_keys = jax.random.split(jax.random.key(seed), 17)
    hot_rows = gaussian(arg_keys[0], (HOT, F), 1.0, 6.0)
    cold_rows = gaussian(arg_keys[1], (COLD_ROWS, F), 1.0, 6.0, ((0, 32),))
    hot_mask = draw_hot_mask(jax.random.fold_in(arg_keys[16], 71), 0)
    hot_id = with_ends(ranked(arg_keys[3], (NODES,), HOT, 2), jax.random.fold_in(arg_keys[3], 3), 0, HOT - 1).astype(jnp.int32)
    cold_owner = draw_cold_owner(jax.random.fold_in(arg_keys[16], 71), 0)
    cold_pos = draw_cold_pos(jax.random.fold_in(arg_keys[16], 71), 0)
    cold_send = with_ends(jax.random.randint(arg_keys[6], (DEVICES, DEVICES * CAP), 0, COLD_DEV), jax.random.fold_in(arg_keys[6], 1), 0, COLD_DEV - 1).astype(jnp.int32)
    adjacency_one = with_ends(jax.random.randint(arg_keys[7], (NODES, K1), 0, L_DEV), jax.random.fold_in(arg_keys[7], 1), 0, L_DEV - 1).astype(jnp.int32)
    adjacency_two = with_ends(jax.random.randint(arg_keys[8], (TARGETS, K2), 0, L_DEV + N_DEV * HCAP), jax.random.fold_in(arg_keys[8], 1), 0, (L_DEV + N_DEV * HCAP) - 1).astype(jnp.int32)
    halo_send = with_ends(jax.random.randint(arg_keys[9], (DEVICES, N_DEV * HCAP), 0, L_DEV), jax.random.fold_in(arg_keys[9], 1), 0, L_DEV - 1).astype(jnp.int32)
    self_first = gaussian(arg_keys[10], (F, H), F ** -0.5, 0.21875)
    neigh_first = gaussian(arg_keys[11], (F, H), F ** -0.5, 0.21875)
    bn_gain = jnp.clip(1.0 + 0.18 * jax.random.normal(arg_keys[12], (H,), jnp.float32), 0.1, 1.9)
    bn_shift = gaussian(arg_keys[13], (H,), 0.5, 3.0, (), jnp.float32)
    self_second = gaussian(arg_keys[14], (H, C), H ** -0.5, 0.1875)
    neigh_second = gaussian(arg_keys[15], (H, C), H ** -0.5, 0.1875)
    return {"hot_rows": hot_rows, "cold_rows": cold_rows, "hot_mask": hot_mask, "hot_id": hot_id, "cold_owner": cold_owner, "cold_pos": cold_pos, "cold_send": cold_send, "adjacency_one": adjacency_one, "adjacency_two": adjacency_two, "halo_send": halo_send, "self_first": self_first, "neigh_first": neigh_first, "bn_gain": bn_gain, "bn_shift": bn_shift, "self_second": self_second, "neigh_second": neigh_second}


epsilon = 1e-05

def gather_mean(table, neighbours, fanout):
    total = jnp.zeros((neighbours.shape[0], table.shape[1]), jnp.float32)
    for column in range(fanout):
        total = total + jnp.take(table, neighbours[:, column], axis=0).astype(jnp.float32)
    return (total / fanout).astype(jnp.bfloat16)

def reference(hot_rows, cold_rows, hot_mask, hot_id, cold_owner, cold_pos, cold_send, adjacency_one, adjacency_two, halo_send, self_first, neigh_first, bn_gain, bn_shift, self_second, neigh_second):
    devices = N_HST * N_DEV

    def first_layer(device):
        start = (device * L_DEV).astype(jnp.int32)
        mask_here = lax.dynamic_slice_in_dim(hot_mask, start, L_DEV)
        hot_here = lax.dynamic_slice_in_dim(hot_id, start, L_DEV)
        owner_here = lax.dynamic_slice_in_dim(cold_owner, start, L_DEV)
        pos_here = lax.dynamic_slice_in_dim(cold_pos, start, L_DEV)
        nbrs_here = lax.dynamic_slice_in_dim(adjacency_one, start, L_DEV)
        slot = cold_send[owner_here, (device * CAP + pos_here).astype(jnp.int32)]
        cold_feat = jnp.take(cold_rows, (owner_here * COLD_DEV + slot).astype(jnp.int32), axis=0)
        hot_feat = jnp.take(hot_rows, hot_here, axis=0)
        features = jnp.where(mask_here[:, None] == 1, hot_feat, cold_feat)
        first_mean = gather_mean(features, nbrs_here, K1)
        return jnp.dot(features, self_first, preferred_element_type=jnp.float32) + jnp.dot(first_mean, neigh_first, preferred_element_type=jnp.float32)
    hidden_pre = lax.map(first_layer, jnp.arange(devices, dtype=jnp.int32))
    mean = lax.optimization_barrier(jnp.mean(hidden_pre, axis=(0, 1)))
    variance = lax.optimization_barrier(jnp.mean(jnp.square(hidden_pre - mean), axis=(0, 1)))
    hidden = jax.nn.relu((hidden_pre - mean) * lax.rsqrt(variance + epsilon) * bn_gain + bn_shift).astype(jnp.bfloat16)
    sends = halo_send.reshape(devices, N_DEV, HCAP)

    def second_layer(device):
        group = device // N_DEV
        lane = device % N_DEV
        peers = (group * N_DEV + jnp.arange(N_DEV, dtype=jnp.int32)).astype(jnp.int32)
        picks = sends[peers, lane]
        boundary = hidden[peers[:, None], picks].reshape(N_DEV * HCAP, H)
        own = lax.dynamic_index_in_dim(hidden, device, 0, keepdims=False)
        table = jnp.concatenate([own, boundary], axis=0)
        nbrs_here = lax.dynamic_slice_in_dim(adjacency_two, (device * B_DEV).astype(jnp.int32), B_DEV)
        second_mean = gather_mean(table, nbrs_here, K2)
        return jnp.dot(own[:B_DEV], self_second, preferred_element_type=jnp.float32) + jnp.dot(second_mean, neigh_second, preferred_element_type=jnp.float32)
    logits = lax.map(second_layer, jnp.arange(devices, dtype=jnp.int32))
    return logits.reshape(devices * B_DEV, C)
```

```python
import functools

import jax
import jax.numpy as jnp
from jax import lax
from jax.experimental import pallas as pl
from jax.experimental.pallas import tpu as pltpu
from jax.sharding import PartitionSpec as P

epsilon = 1e-05
LANES = 128
MIB = 1024 * 1024
MESH = pl.DeviceIdType.MESH
BF16, F32, I32 = jnp.bfloat16, jnp.float32, jnp.int32


def dot(a, b):
    return jnp.dot(a, b, preferred_element_type=F32)


def dot_nt(a, b):
    return lax.dot_general(a, b, (((1,), (1,)), ((), ())), preferred_element_type=F32)


def hot_where(match, value=1.0):
    return jnp.where(match, value, 0.0).astype(BF16)


def iota(shape, axis):
    return lax.broadcasted_iota(I32, shape, axis)


def spread(column):
    return jnp.broadcast_to(column, (column.shape[0], LANES))


def one_hot_tiles(wide, tiles):
    lane = iota(wide.shape, 1)
    return jnp.concatenate([hot_where(wide == lane + LANES * t) for t in range(tiles)], axis=1)


def look_up(table, index):
    low, high = index & (LANES - 1), index >> 7
    out = jnp.zeros_like(index)
    for t in range(table.shape[0]):
        row = jnp.broadcast_to(table[t : t + 1, :], index.shape)
        out = jnp.where(high == t, jnp.take_along_axis(row, low, axis=1, mode="promise_in_bounds"), out)
    return out


def running_count(flags):
    tiles = flags.shape[0]
    marks = flags.astype(BF16)
    before = hot_where(iota((LANES, LANES), 0) < iota((LANES, LANES), 1))
    within = dot(marks, before)
    totals = dot(marks, jnp.ones((LANES, LANES), BF16)).astype(BF16)
    above = hot_where(iota((tiles, tiles), 1) < iota((tiles, tiles), 0))
    return (within + dot(above, totals)).astype(I32)


def digits_of(slots, valid, words):
    low, high = slots & (LANES - 1), slots >> 7
    parts = [low.astype(F32)]
    for word in range(words):
        here = valid & ((high >> 3) == word)
        parts.append(jnp.where(here, (jnp.int32(1) << ((high & 7) * 4)), 0).astype(F32))
    return jnp.concatenate(parts, axis=0).astype(BF16)


def count_block(digits_ref, start, rows, fanout, lines, words, tiles, put):
    digits = digits_ref[pl.ds(start, rows), :]
    lane = iota((rows, LANES), 1)
    sums = [jnp.zeros((rows, LANES), I32) for _ in range(words)]
    for k in range(fanout):
        match = spread(digits[:, k : k + 1]) == lane
        for word in range(words):
            at = (word + 1) * lines + k
            sums[word] = sums[word] + jnp.where(match, spread(digits[:, at : at + 1]), 0)
    for t in range(tiles):
        put(t, ((sums[t // 8] >> (4 * (t % 8))) & 15).astype(F32).astype(BF16))


def program(dims, hot_hbm, cold_hbm, mask_ref, hot_id_ref, owner_ref, pos_ref, send_ref, near_ref, next_ref,
            halo_ref, self_hbm, neigh_hbm, gain_ref, shift_ref, self2_ref, neigh2_ref, out_ref,
            cold, outgoing, arrived, hot, extra, counts, edge_counts, total, edge_total, pre, last_counts,
            self_w, neigh_w, edge_out, edge_in, wide, used, digits, slots_near, slots_next, rows, tables, square,
            chunk_rows, stat_own, stat_near, stat_part, stat_far,
            load, send, recv, send_edge, recv_edge, edge_copy, send_near, recv_near, send_far, recv_far):
    hosts, within, fanout, fanout2, total_rows = dims
    devices = hosts * within
    slots, width = outgoing.shape
    units = pre.shape[1]
    cap = slots // devices
    half = within // 2
    tiles = slots // LANES
    chunk, chunks = counts.shape[2], counts.shape[0]
    edge = edge_out.shape[0]
    share = edge // within
    targets = out_ref.shape[1]
    host, lane = lax.axis_index("hst"), lax.axis_index("dev")
    me = host * within + lane
    side = lane // half

    def at(peer):
        return {"hst": peer // within, "dev": lax.rem(peer, within)}

    loads = [
        pltpu.make_async_copy(source, target, load.at[i])
        for i, (source, target) in enumerate(
            [(cold_hbm, cold), (hot_hbm, hot), (self_hbm, self_w), (neigh_hbm, neigh_w)]
        )
    ]
    loads[0].start()

    barrier = pltpu.get_barrier_semaphore()

    def greet(away, carry):
        pl.semaphore_signal(barrier, inc=1, device_id=at(lax.rem(me + away, devices)), device_id_type=MESH)
        return carry

    lax.fori_loop(1, devices, greet, 0)

    square[...] = jnp.zeros_like(square)
    for t in range(tiles):
        square[t : t + 1, :] = send_ref[:, t * LANES : (t + 1) * LANES].astype(F32)
    turned = square[...].T.astype(I32)
    for t in range(tiles):
        wide[t * LANES : (t + 1) * LANES, :] = spread(turned[:, t : t + 1])
    loads[0].wait()

    def pick(step, carry):
        here = pl.ds(pl.multiple_of(step * 256, 256), 256)
        outgoing[here, :] = dot(one_hot_tiles(wide[here, :], cold.shape[0] // LANES), cold[...]).astype(BF16)
        return carry

    lax.fori_loop(0, slots // 256, pick, 0)
    pl.semaphore_wait(barrier, devices - 1)

    def block(peer):
        return pl.ds(pl.multiple_of(peer * cap, cap), cap)

    def row_copy(peer):
        away = lax.rem(peer - me + devices, devices)
        return pltpu.make_async_remote_copy(
            src_ref=outgoing.at[block(peer)], dst_ref=arrived.at[block(me)],
            send_sem=send.at[away], recv_sem=recv.at[away], device_id=at(peer), device_id_type=MESH,
        )

    def peer_of(step, flip, towards):
        h = lax.rem(host + (step // half) * towards + hosts, hosts)
        return h * within + lax.rem(side + flip, 2) * half + lax.rem(lane + step, half)

    def start_far(step, carry):
        row_copy(peer_of(step, 1, 1)).start()
        return carry

    def start_near(step, carry):
        row_copy(peer_of(step, 0, 1)).start()
        return carry

    lax.fori_loop(0, hosts * half, start_far, 0)
    lax.fori_loop(1, hosts * half, start_near, 0)
    for copy in loads[1:]:
        copy.start()
    arrived[block(me), :] = outgoing[block(me), :]

    def to_table(row, i):
        for t in range(tiles):
            tables[i, t : t + 1, :] = row[:, t * LANES : (t + 1) * LANES]

    def to_row(table, i):
        for t in range(tiles):
            rows[i : i + 1, t * LANES : (t + 1) * LANES] = table[t : t + 1, :]

    cold_node = mask_ref[...] != 1
    key = jnp.where(cold_node, owner_ref[...] * cap + pos_ref[...], -1)
    to_table(key, 0)
    key_table = tables[0]
    high = hot_where((key >> 7) == iota((tiles, slots), 0))
    low = hot_where((key & (LANES - 1)) == iota((LANES, slots), 0))
    taken = dot_nt(high, low) > 0.5
    free_rank = running_count(jnp.where(taken, 0.0, 1.0))
    to_row(jnp.where(taken, -1, free_rank), 0)
    rank = rows[0:1, :]
    slot = iota((1, slots), 1)
    high = (rank >> 7) == iota((tiles, slots), 0)
    low = hot_where((rank & (LANES - 1)) == iota((LANES, slots), 0))
    free_slot = dot_nt(hot_where(high, (slot >> 7).astype(F32)), low).astype(I32) * LANES
    free_slot = free_slot + dot_nt(hot_where(high, (slot & (LANES - 1)).astype(F32)), low).astype(I32)
    hot_rank = running_count(jnp.where(key_table < 0, 1.0, 0.0))
    tables[1] = jnp.where(key_table < 0, look_up(free_slot, hot_rank), key_table)
    to_row(tables[1], 1)

    slots_near[...] = jnp.zeros_like(slots_near)
    slots_near[0:fanout, :] = near_ref[...]
    slots_next[...] = jnp.zeros_like(slots_next)
    slots_next[0:fanout2, :] = next_ref[...]
    lines, lines2 = slots_near.shape[0], slots_next.shape[0]

    def map_near(step, carry):
        here = pl.ds(pl.multiple_of(step * LANES, LANES), LANES)
        slots_near[:, here] = look_up(tables[1], slots_near[:, here])
        return carry

    lax.fori_loop(0, slots // LANES, map_near, 0)

    def map_next(step, carry):
        here = pl.ds(pl.multiple_of(step * LANES, LANES), LANES)
        index = slots_next[:, here]
        slots_next[:, here] = jnp.where(index < slots, look_up(tables[1], index), index)
        return carry

    lax.fori_loop(0, targets // LANES, map_next, 0)
    words, words2 = -(-tiles // 8), -(-(tiles + edge // LANES) // 8)
    near_digits = digits_of(slots_near[...], iota((lines, slots), 0) < fanout, words)
    own = jnp.where(cold_node, 0, hot_id_ref[...])
    own_lines = jnp.concatenate(
        [
            jnp.broadcast_to((own >> 7).astype(F32), (lines, slots)),
            jnp.broadcast_to((own & (LANES - 1)).astype(F32), (lines, slots)),
            jnp.broadcast_to(jnp.where(cold_node, 0.0, 1.0), (lines, slots)),
        ],
        axis=0,
    ).astype(BF16)
    near_digits = jnp.concatenate([near_digits, own_lines], axis=0)
    node_slot = rows[1:2, :]
    first_own = (words + 1) * lines

    for copy in loads[1:]:
        copy.wait()

    def build(step, carry):
        start = pl.multiple_of(step * 256, 256)
        here = pl.ds(start, 256)
        mine = hot_where(node_slot == iota((256, slots), 0) + start)
        found = dot_nt(mine, near_digits).astype(I32)
        digits[:, 0 : found.shape[1]] = found
        is_hot = found[:, first_own + 2 * lines : first_own + 2 * lines + 1] > 0
        row = found[:, first_own : first_own + 1] * LANES + found[:, first_own + lines : first_own + lines + 1]
        row = spread(jnp.where(is_hot, row, -1))
        used[here, :] = row
        for part in range(4):
            size = hot.shape[0] // 4
            picks = one_hot_tiles(row - part * size, size // LANES)
            product = dot(picks, hot[part * size : (part + 1) * size, :])
            got = product if part == 0 else got + product
        extra[here, :] = got.astype(BF16)

        def some(part, carry):
            at_row = pl.multiple_of(part * 32, 32)

            def put(t, value):
                counts[t * LANES // chunk, pl.ds(start + at_row, 32),
                       t * LANES % chunk : t * LANES % chunk + LANES] = value

            count_block(digits, at_row, 32, fanout, lines, words, tiles, put)
            return carry

        lax.fori_loop(0, 256 // 32, some, 0)
        return carry

    lax.fori_loop(0, slots // 256, build, 0)

    for t in range(edge // LANES):
        index = jnp.broadcast_to(halo_ref[:, t * LANES : (t + 1) * LANES], (8, LANES))
        index = look_up(tables[1], index)
        pair = jnp.concatenate([(index >> 7).astype(F32), (index & (LANES - 1)).astype(F32)], axis=0).astype(BF16)
        eye = hot_where(iota((LANES, LANES), 0) == iota((LANES, LANES), 1))
        found = dot_nt(eye, pair).astype(I32)
        column = spread(found[:, 0:1] * LANES + found[:, 8:9])
        picks = one_hot_tiles(column, tiles)
        for c in range(chunks):
            edge_counts[c, t * LANES : (t + 1) * LANES, :] = dot(picks, counts[c]).astype(BF16)
            edge_counts[c, edge + t * LANES : edge + (t + 1) * LANES, :] = picks[:, c * chunk : (c + 1) * chunk]

    for t in range(targets // LANES):
        there = slice(t * LANES, (t + 1) * LANES)
        index = slots_next[:, there]
        parts = digits_of(index, iota((lines2, LANES), 0) < fanout2, words2)
        index = jnp.broadcast_to(tables[1, t : t + 1, :], (16, LANES))
        pair = jnp.concatenate([(index >> 7).astype(F32), (index & (LANES - 1)).astype(F32)], axis=0).astype(BF16)
        parts = jnp.concatenate([parts, pair], axis=0)
        eye = hot_where(iota((LANES, LANES), 0) == iota((LANES, LANES), 1))
        found = dot_nt(eye, parts).astype(I32)
        digits[0:LANES, 0 : found.shape[1]] = found
        at_own = (words2 + 1) * lines2
        column = spread(found[:, at_own : at_own + 1] * LANES + found[:, at_own + 16 : at_own + 17])
        last_counts[targets + t * LANES : targets + (t + 1) * LANES, 0:slots] = one_hot_tiles(column, tiles)

        def some(part, carry):
            at_row = pl.multiple_of(part * 32, 32)

            def put(tile, value):
                last_counts[pl.ds(t * LANES + at_row, 32), tile * LANES : (tile + 1) * LANES] = value

            count_block(digits, at_row, 32, fanout2, lines2, words2, tiles + edge // LANES, put)
            return carry

        lax.fori_loop(0, LANES // 32, some, 0)

    total[...] = jnp.zeros_like(total)
    edge_total[...] = jnp.zeros_like(edge_total)

    def arrive(step, carry):
        h = lax.rem(host - lax.rem(step, hosts) + hosts, hosts)
        which = h * 2 + lax.rem(side + step // hosts, 2)

        def await_one(q, carry):
            peer = which * half + q

            @pl.when(peer != me)
            def _():
                away = lax.rem(me - peer + devices, devices)
                pltpu.make_async_remote_copy(
                    src_ref=outgoing.at[block(me)], dst_ref=arrived.at[block(peer)],
                    send_sem=send.at[away], recv_sem=recv.at[away], device_id=at(peer), device_id_type=MESH,
                ).wait_recv()

            return carry

        lax.fori_loop(0, half, await_one, 0)
        here = pl.ds(pl.multiple_of(which * chunk, chunk), chunk)
        mine = jnp.concatenate([used[here, :]] * (width // LANES), axis=1) < 0
        chunk_rows[...] = jnp.where(mine, arrived[here, :].astype(F32), extra[here, :].astype(F32)).astype(BF16)
        pre[here, :] = dot(chunk_rows[...], self_w[...])
        edge_total[...] += dot(edge_counts[which], chunk_rows[...])

        def gather(part, carry):
            there = pl.ds(pl.multiple_of(part * 512, 512), 512)
            total[there, :] += dot(counts[which, there, :], chunk_rows[...])
            return carry

        lax.fori_loop(0, slots // 512, gather, 0)
        return carry

    lax.fori_loop(0, chunks, arrive, 0)

    edge_mean = (edge_total[0:edge, :] * (1.0 / fanout)).astype(BF16)
    edge_pre = dot(edge_total[edge : 2 * edge, :].astype(BF16), self_w[...]) + dot(edge_mean, neigh_w[...])
    centre = jnp.mean(edge_pre, axis=0, keepdims=True)
    edge_out[...] = (edge_pre - centre).astype(BF16)

    def part_of(peer):
        return pl.ds(pl.multiple_of(peer * share, share), share)

    edge_copies = []
    for away in range(1, within):
        peer = lax.rem(lane + away, within)
        edge_copies.append(pltpu.make_async_remote_copy(
            src_ref=edge_out.at[part_of(peer)], dst_ref=edge_in.at[part_of(lane)],
            send_sem=send_edge.at[away - 1], recv_sem=recv_edge.at[away - 1],
            device_id={"dev": peer}, device_id_type=MESH,
        ))
        edge_copies[-1].start()
    edge_in[part_of(lane), :] = edge_out[part_of(lane), :]

    def finish(step, sums):
        here = pl.ds(pl.multiple_of(step * 256, 256), 256)
        mean = (total[here, :] * (1.0 / fanout)).astype(BF16)
        value = pre[here, :] + dot(mean, neigh_w[...])
        pre[here, :] = value
        return sums[0] + jnp.sum(value, axis=0, keepdims=True), sums[1] + jnp.sum(value * value, axis=0, keepdims=True)

    zero = jnp.zeros((1, units), F32)
    first, second = lax.fori_loop(0, slots // 256, finish, (zero, zero))
    stat_own[...] = jnp.concatenate([first, second, centre, zero], axis=0)

    def exchange(source, landing, axis, index, size, send_sem, recv_sem):
        copies = []
        for away in range(1, size):
            copies.append(pltpu.make_async_remote_copy(
                src_ref=source, dst_ref=landing.at[away - 1], send_sem=send_sem.at[away - 1],
                recv_sem=recv_sem.at[away - 1], device_id={axis: lax.rem(index + away, size)},
                device_id_type=MESH,
            ))
            copies[-1].start()
        for copy in copies:
            copy.wait()
        value = source[...]
        for away in range(1, size):
            value = value + landing[away - 1]
        return value

    stat_part[...] = exchange(stat_own, stat_near, "dev", lane, within, send_near, recv_near)
    sums = exchange(stat_part, stat_far, "hst", host, hosts, send_far, recv_far)
    mean = sums[0:1, :] / total_rows
    variance = sums[1:2, :] / total_rows - mean * mean
    scale = lax.rsqrt(variance + epsilon) * gain_ref[...]
    shift = shift_ref[...]

    def normal(step, carry):
        here = pl.ds(pl.multiple_of(step * 256, 256), 256)
        hidden = jnp.maximum((pre[here, :] - mean) * scale + shift, 0.0).astype(BF16)
        for c in range(units // chunk):
            counts[c, here, :] = hidden[:, c * chunk : (c + 1) * chunk]
        return carry

    lax.fori_loop(0, slots // 256, normal, 0)
    for copy in edge_copies:
        copy.wait()
    for away in range(within):
        there = part_of(lax.rem(lane - away + within, within))
        origin = centre if away == 0 else stat_near[away - 1][2:3, :]
        value = edge_in[there, :].astype(F32) + (origin - mean)
        edge_in[there, :] = jnp.maximum(value * scale + shift, 0.0).astype(BF16)
    out_ref[...] = jnp.zeros_like(out_ref)

    def second_layer(c, carry):
        there = pl.ds(pl.multiple_of(c * chunk, chunk), chunk)
        both = dot(last_counts[:, 0:slots], counts[c])
        near = both[0:targets, :] + dot(last_counts[0:targets, slots:], edge_in[:, there])
        near = (near * (1.0 / fanout2)).astype(BF16)
        out_ref[...] += dot_nt(neigh2_ref[:, there], near) + dot_nt(self2_ref[:, there], both[targets:, :].astype(BF16))
        return carry

    lax.fori_loop(0, units // chunk, second_layer, 0)

    def drain(away, carry):
        row_copy(lax.rem(me + away, devices)).wait_send()
        return carry

    lax.fori_loop(1, devices, drain, 0)


def local(hot_rows, cold_rows, hot_mask, hot_id, cold_owner, cold_pos, cold_send, adjacency_one, adjacency_two,
          halo_send, self_first, neigh_first, bn_gain, bn_shift, self_second, neigh_second):
    hosts, within = lax.axis_size("hst"), lax.axis_size("dev")
    devices = hosts * within
    nodes, fanout = adjacency_one.shape
    targets, fanout2 = adjacency_two.shape
    slots, edge = cold_send.shape[1], halo_send.shape[1]
    width, units = self_first.shape
    classes = self_second.shape[1]
    assert slots == nodes
    chunk = slots // devices * (within // 2)
    chunks = slots // chunk
    lines, lines2 = -(-fanout // 16) * 16, -(-fanout2 // 16) * 16
    tiles = slots // LANES
    any_space, vmem = pl.BlockSpec(memory_space=pl.ANY), pl.BlockSpec(memory_space=pltpu.VMEM)
    dma = pltpu.SemaphoreType.DMA
    out = pl.pallas_call(
        functools.partial(program, (hosts, within, fanout, fanout2, nodes * devices)),
        in_specs=[any_space] * 2 + [vmem] * 8 + [any_space] * 2 + [vmem] * 4,
        out_specs=vmem,
        out_shape=jax.ShapeDtypeStruct((classes, targets), F32),
        scratch_shapes=[
            pltpu.VMEM(cold_rows.shape, BF16),
            pltpu.VMEM((slots, width), BF16),
            pltpu.VMEM((slots, width), BF16),
            pltpu.VMEM(hot_rows.shape, BF16),
            pltpu.VMEM((slots, width), BF16),
            pltpu.VMEM((chunks, slots, chunk), BF16),
            pltpu.VMEM((chunks, 2 * edge, chunk), BF16),
            pltpu.VMEM((slots, width), F32),
            pltpu.VMEM((2 * edge, width), F32),
            pltpu.VMEM((slots, units), F32),
            pltpu.VMEM((2 * targets, slots + edge), BF16),
            pltpu.VMEM((width, units), BF16),
            pltpu.VMEM((width, units), BF16),
            pltpu.VMEM((edge, units), BF16),
            pltpu.VMEM((edge, units), BF16),
            pltpu.VMEM((slots, LANES), I32),
            pltpu.VMEM((slots, LANES), I32),
            pltpu.VMEM((256, LANES), I32),
            pltpu.VMEM((lines, slots), I32),
            pltpu.VMEM((lines2, targets), I32),
            pltpu.VMEM((8, slots), I32),
            pltpu.VMEM((2, tiles, LANES), I32),
            pltpu.VMEM((LANES, LANES), F32),
            pltpu.VMEM((chunk, width), BF16),
            pltpu.VMEM((4, units), F32),
            pltpu.VMEM((within - 1, 4, units), F32),
            pltpu.VMEM((4, units), F32),
            pltpu.VMEM((hosts - 1, 4, units), F32),
            dma((4,)),
            dma((devices,)),
            dma((devices,)),
            dma((within - 1,)),
            dma((within - 1,)),
            dma,
            dma((within - 1,)),
            dma((within - 1,)),
            dma((hosts - 1,)),
            dma((hosts - 1,)),
        ],
        compiler_params=pltpu.CompilerParams(
            collective_id=0, has_side_effects=True, vmem_limit_bytes=63 * MIB
        ),
        name="sage",
    )(
        hot_rows, cold_rows, hot_mask[None, :], hot_id[None, :], cold_owner[None, :], cold_pos[None, :], cold_send,
        adjacency_one.T, adjacency_two.T, halo_send, self_first, neigh_first, bn_gain[None, :], bn_shift[None, :],
        self_second.T, neigh_second.T,
    )
    return out.T


def solution(mesh):
    owned, split, copied = P(("hst", "dev"), None), P(("hst", "dev")), P()
    placed = (copied, owned) + (split,) * 4 + (owned,) * 4 + (copied,) * 6
    return jax.shard_map(local, mesh=mesh, in_specs=placed, out_specs=owned, check_vma=False)
```

```python
import functools
import math

import jax
import jax.numpy as jnp
from jax import lax
from jax.experimental import pallas as pl
from jax.experimental.pallas import tpu as pltpu
from jax.sharding import PartitionSpec as P

epsilon = 1e-05
LANES = 128
MIB = 1024 * 1024
SHARES = 4
MESH = pl.DeviceIdType.MESH
BF16, F32, I32 = jnp.bfloat16, jnp.float32, jnp.int32


def dot(a, b):
    return jnp.dot(a, b, preferred_element_type=F32)


def dot_nt(a, b):
    return lax.dot_general(a, b, (((1,), (1,)), ((), ())), preferred_element_type=F32)


def hot_where(match, value=1.0):
    return jnp.where(match, value, 0.0).astype(BF16)


def iota(shape, axis):
    return lax.broadcasted_iota(I32, shape, axis)


def spread(column):
    return jnp.broadcast_to(column, (column.shape[0], LANES))


def one_hot_tiles(wide, tiles):
    lane = iota(wide.shape, 1)
    return jnp.concatenate([hot_where(wide == lane + LANES * t) for t in range(tiles)], axis=1)


def look_up(table, index):
    low, high = index & (LANES - 1), index >> 7
    out = jnp.zeros_like(index)
    for t in range(table.shape[0]):
        row = jnp.broadcast_to(table[t : t + 1, :], index.shape)
        out = jnp.where(high == t, jnp.take_along_axis(row, low, axis=1, mode="promise_in_bounds"), out)
    return out


def running_count(flags):
    tiles = flags.shape[0]
    marks = flags.astype(BF16)
    before = hot_where(iota((LANES, LANES), 0) < iota((LANES, LANES), 1))
    within = dot(marks, before)
    totals = dot(marks, jnp.ones((LANES, LANES), BF16)).astype(BF16)
    above = hot_where(iota((tiles, tiles), 1) < iota((tiles, tiles), 0))
    return (within + dot(above, totals)).astype(I32)


def turned(row):
    return jnp.broadcast_to(row, (LANES, LANES)).T


def inverse_of(row, tiles, value):
    high = (row >> 7) == iota((tiles, row.shape[1]), 0)
    low = hot_where((row & (LANES - 1)) == iota((LANES, row.shape[1]), 0))
    upper = dot_nt(hot_where(high, (value >> 7).astype(F32)), low).astype(I32)
    lower = dot_nt(hot_where(high, (value & (LANES - 1)).astype(F32)), low).astype(I32)
    return upper * LANES + lower


def count_tile(index, fanout, tiles, lows, nibbles, put):
    words = -(-tiles // 8)
    high = index >> 7
    lows[...] = index & (LANES - 1)
    for word in range(words):
        nibbles[word] = jnp.where((high >> 3) == word, jnp.int32(1) << ((high & 7) * 4), 0)
    part = 32
    sums = [[] for _ in range(words)]
    for start in range(0, LANES, part):
        place = iota((part, LANES), 0) + start
        held = [jnp.zeros((part, LANES), I32) for _ in range(words)]
        for k in range(fanout):
            match = jnp.broadcast_to(lows[k : k + 1, :], (part, LANES)) == place
            for word in range(words):
                more = jnp.broadcast_to(nibbles[word, k : k + 1, :], (part, LANES))
                held[word] = held[word] + jnp.where(match, more, 0)
        for word in range(words):
            sums[word].append(held[word])
    for word in range(words):
        across = jnp.concatenate(sums[word], axis=0).T
        for t in range(word * 8, min(tiles, word * 8 + 8)):
            put(t, ((across >> (4 * (t % 8))) & 15).astype(F32).astype(BF16))


def program(dims, hot_hbm, cold_hbm, mask_hbm, hot_id_hbm, owner_hbm, pos_hbm, send_hbm, near_hbm, next_hbm,
            halo_hbm, self_hbm, neigh_hbm, gain_hbm, shift_hbm, self2_hbm, neigh2_hbm, out_ref,
            mask_ref, hot_id_ref, owner_ref, pos_ref, send_ref, near_ref, next_ref, halo_ref, gain_ref, shift_ref,
            self2_ref, neigh2_ref,
            cold, outgoing, arrived, hot, extra, counts, edge_counts, total, edge_total, pre, last_counts,
            self_w, neigh_w, edge_out, edge_in, wide, slots_near, slots_sorted, slots_next, rows, tables, lows, nibbles,
            chunk_rows, stat_own, stat_near, stat_part, stat_far,
            load, send, recv, send_edge, recv_edge, send_near, recv_near, send_far, recv_far):
    hosts, within, fanout, fanout2, total_rows = dims
    devices = hosts * within
    slots, width = outgoing.shape
    units = pre.shape[1]
    cap = slots // devices
    half = within // 2
    tiles = slots // LANES
    chunk, chunks = counts.shape[2], counts.shape[0]
    edge = edge_out.shape[0]
    share = edge // within
    targets = out_ref.shape[1]
    host, lane = lax.axis_index("hst"), lax.axis_index("dev")
    me = host * within + lane
    side = lane // half

    def at(peer):
        return {"hst": peer // within, "dev": lax.rem(peer, within)}

    loads = [
        pltpu.make_async_copy(source, target, load.at[i])
        for i, (source, target) in enumerate(
            [
                (send_hbm, send_ref), (cold_hbm, cold), (mask_hbm, mask_ref), (hot_id_hbm, hot_id_ref),
                (owner_hbm, owner_ref), (pos_hbm, pos_ref), (near_hbm, near_ref), (next_hbm, next_ref),
                (halo_hbm, halo_ref), (gain_hbm, gain_ref), (shift_hbm, shift_ref), (self2_hbm, self2_ref),
                (neigh2_hbm, neigh2_ref), (hot_hbm, hot), (self_hbm, self_w), (neigh_hbm, neigh_w),
            ]
        )
    ]
    early, middle, late = loads[:2], loads[2:13], loads[13:]
    for copy in early:
        copy.start()

    barrier = pltpu.get_barrier_semaphore()

    def greet(away, carry):
        pl.semaphore_signal(barrier, inc=1, device_id=at(lax.rem(me + away, devices)), device_id_type=MESH)
        return carry

    lax.fori_loop(1, devices, greet, 0)

    def block(peer):
        return pl.ds(pl.multiple_of(peer * cap, cap), cap)

    def row_copy(peer):
        away = lax.rem(peer - me + devices, devices)
        return pltpu.make_async_remote_copy(
            src_ref=outgoing.at[block(peer)], dst_ref=arrived.at[block(me)],
            send_sem=send.at[away], recv_sem=recv.at[away], device_id=at(peer), device_id_type=MESH,
        )

    def chunk_at(step, towards):
        h = lax.rem(host + lax.rem(step, hosts) * towards + hosts, hosts)
        return h * 2 + lax.rem(side + 1 + step // hosts, 2)

    def pick(step):
        begin = chunk_at(step, 1) * chunk
        columns = [
            turned(send_ref[:, pl.ds(pl.multiple_of(begin + t, LANES), LANES)]) for t in range(0, chunk, LANES)
        ]
        picks = one_hot_tiles(jnp.concatenate(columns, axis=0), cold.shape[0] // LANES)
        outgoing[pl.ds(pl.multiple_of(begin, chunk), chunk), :] = dot(picks, cold[...]).astype(BF16)

    def start(step):
        def start_one(q, carry):
            peer = chunk_at(step, 1) * half + lax.rem(lane + q, half)

            @pl.when(peer != me)
            def _():
                row_copy(peer).start()

            return carry

        lax.fori_loop(0, half, start_one, 0)

    def pick_and_start(step, carry):
        pick(step)
        start(step)
        return carry

    for copy in early:
        copy.wait()
    pick(0)
    pl.semaphore_wait(barrier, devices - 1)
    start(0)
    lax.fori_loop(1, chunks, pick_and_start, 0)
    for copy in middle + late:
        copy.start()
    arrived[block(me), :] = outgoing[block(me), :]

    def to_table(row, i):
        for t in range(tiles):
            tables[i, t : t + 1, :] = row[:, t * LANES : (t + 1) * LANES]

    def to_row(table, i):
        for t in range(tiles):
            rows[i : i + 1, t * LANES : (t + 1) * LANES] = table[t : t + 1, :]

    for copy in middle:
        copy.wait()
    cold_node = mask_ref[...] != 1
    key = jnp.where(cold_node, owner_ref[...] * cap + pos_ref[...], -1)
    to_table(key, 0)
    key_table = tables[0]
    high = hot_where((key >> 7) == iota((tiles, slots), 0))
    low = hot_where((key & (LANES - 1)) == iota((LANES, slots), 0))
    taken = dot_nt(high, low) > 0.5
    free_rank = running_count(jnp.where(taken, 0.0, 1.0))
    to_row(jnp.where(taken, -1, free_rank), 0)
    free_slot = inverse_of(rows[0:1, :], tiles, iota((1, slots), 1))
    hot_rank = running_count(jnp.where(key_table < 0, 1.0, 0.0))
    tables[1] = jnp.where(key_table < 0, look_up(free_slot, hot_rank), key_table)
    to_row(tables[1], 1)

    to_row(inverse_of(rows[1:2, :], tiles, iota((1, slots), 1)), 2)

    lines = slots_near.shape[0]
    slots_near[...] = jnp.zeros_like(slots_near)
    slots_near[0:fanout, :] = near_ref[...]
    slots_next[...] = jnp.zeros_like(slots_next)
    slots_next[0:fanout2, :] = next_ref[...]

    def map_near(step, carry):
        here = pl.ds(pl.multiple_of(step * LANES, LANES), LANES)
        slots_near[:, here] = look_up(tables[1], slots_near[:, here])
        return carry

    lax.fori_loop(0, tiles, map_near, 0)
    slots_near[fanout : fanout + 1, :] = jnp.where(cold_node, -1, hot_id_ref[...])

    def sort_near(step, carry):
        here = pl.ds(pl.multiple_of(step * LANES, LANES), LANES)
        node = jnp.broadcast_to(rows[2:3, here], (lines, LANES))
        low, high = node & (LANES - 1), node >> 7
        out = jnp.zeros_like(node)
        for t in range(tiles):
            part = slots_near[:, t * LANES : (t + 1) * LANES]
            out = jnp.where(high == t, jnp.take_along_axis(part, low, axis=1, mode="promise_in_bounds"), out)
        slots_sorted[:, here] = out
        wide[here, :] = turned(out[fanout : fanout + 1, :])
        return carry

    lax.fori_loop(0, tiles, sort_near, 0)

    def map_next(step, carry):
        here = pl.ds(pl.multiple_of(step * LANES, LANES), LANES)
        index = slots_next[:, here]
        slots_next[:, here] = jnp.where(index < slots, look_up(tables[1], index), index)
        return carry

    lax.fori_loop(0, targets // LANES, map_next, 0)
    for copy in late:
        copy.wait()

    def build(step, carry):
        first = pl.multiple_of(step * 256, 256)
        here = pl.ds(first, 256)
        for part in range(4):
            size = hot.shape[0] // 4
            picks = one_hot_tiles(wide[here, :] - part * size, size // LANES)
            product = dot(picks, hot[part * size : (part + 1) * size, :])
            got = product if part == 0 else got + product
        extra[here, :] = got.astype(BF16)
        for part in range(256 // LANES):
            there = pl.ds(pl.multiple_of(first + part * LANES, LANES), LANES)

            def put(t, value):
                counts[t * LANES // chunk, there, t * LANES % chunk : t * LANES % chunk + LANES] = value

            count_tile(slots_sorted[:, there], fanout, tiles, lows, nibbles, put)
        return carry

    lax.fori_loop(0, slots // 256, build, 0)

    for t in range(edge // LANES):
        index = jnp.broadcast_to(halo_ref[:, t * LANES : (t + 1) * LANES], (8, LANES))
        picks = one_hot_tiles(turned(look_up(tables[1], index)[0:1, :]), tiles)
        last_counts[t * LANES : (t + 1) * LANES, 0:slots] = picks
        for c in range(chunks):
            edge_counts[c, edge + t * LANES : edge + (t + 1) * LANES, :] = picks[:, c * chunk : (c + 1) * chunk]

    def count_edge(c, carry):
        edge_counts[c, 0:edge, :] = dot(last_counts[0:edge, 0:slots], counts[c]).astype(BF16)
        return carry

    lax.fori_loop(0, chunks, count_edge, 0)

    def count_target(step, carry):
        there = pl.ds(pl.multiple_of(step * LANES, LANES), LANES)

        def put(t, value):
            last_counts[there, t * LANES : (t + 1) * LANES] = value

        count_tile(slots_next[:, there], fanout2, tiles + edge // LANES, lows, nibbles, put)
        own = pl.ds(pl.multiple_of(targets + step * LANES, LANES), LANES)
        last_counts[own, 0:slots] = one_hot_tiles(turned(rows[1:2, there]), tiles)
        return carry

    lax.fori_loop(0, targets // LANES, count_target, 0)

    total[...] = jnp.zeros_like(total)
    edge_total[...] = jnp.zeros_like(edge_total)

    def take(step):
        which = chunk_at(lax.rem(step + hosts, chunks), -1)

        def await_one(q, carry):
            peer = which * half + q

            @pl.when(peer != me)
            def _():
                away = lax.rem(me - peer + devices, devices)
                pltpu.make_async_remote_copy(
                    src_ref=outgoing.at[block(me)], dst_ref=arrived.at[block(peer)],
                    send_sem=send.at[away], recv_sem=recv.at[away], device_id=at(peer), device_id_type=MESH,
                ).wait_recv()

            return carry

        lax.fori_loop(0, half, await_one, 0)
        here = pl.ds(pl.multiple_of(which * chunk, chunk), chunk)
        mine = jnp.concatenate([wide[here, :]] * (width // LANES), axis=1) < 0
        chunk_rows[...] = jnp.where(mine, arrived[here, :].astype(F32), extra[here, :].astype(F32)).astype(BF16)
        edge_total[...] += dot(edge_counts[which], chunk_rows[...])

    def work(step):
        which = chunk_at(lax.rem(step + hosts, chunks), -1)
        here = pl.ds(pl.multiple_of(which * chunk, chunk), chunk)
        pre[here, :] = dot(chunk_rows[...], self_w[...])

        def gather(part, carry):
            there = pl.ds(pl.multiple_of(part * 512, 512), 512)
            total[there, :] += dot(counts[which, there, :], chunk_rows[...])
            return carry

        lax.fori_loop(0, slots // 512, gather, 0)

    def arrive(step, carry):
        take(step)
        work(step)
        return carry

    lax.fori_loop(0, chunks - 1, arrive, 0)
    take(chunks - 1)

    edge_mean = (edge_total[0:edge, :] * (1.0 / fanout)).astype(BF16)
    edge_pre = dot(edge_total[edge : 2 * edge, :].astype(BF16), self_w[...]) + dot(edge_mean, neigh_w[...])
    centre = jnp.mean(edge_pre, axis=0, keepdims=True)
    edge_out[...] = (edge_pre - centre).astype(BF16)

    def part_of(peer):
        return pl.ds(pl.multiple_of(peer * share, share), share)

    def edge_copy(peer):
        away = lax.rem(peer - lane + within, within)
        return pltpu.make_async_remote_copy(
            src_ref=edge_out.at[part_of(peer)], dst_ref=edge_in.at[part_of(lane)],
            send_sem=send_edge.at[away], recv_sem=recv_edge.at[away],
            device_id={"dev": peer}, device_id_type=MESH,
        )

    near_peers = [side * half + lax.rem(lane + q, half) for q in range(1, half)]
    far_peers = [lax.rem(side + 1, 2) * half + lax.rem(lane + q, half) for q in range(half)]
    for peer in far_peers[: half // 2] + near_peers:
        edge_copy(peer).start()
    edge_in[part_of(lane), :] = edge_out[part_of(lane), :]
    work(chunks - 1)

    shares = stat_own.shape[0]
    columns = units // shares
    near_copies, far_copies = {}, {}

    def swap(source, landing, axis, index, size, send_sem, recv_sem):
        copies = []
        for away in range(1, size):
            copies.append(pltpu.make_async_remote_copy(
                src_ref=source, dst_ref=landing.at[away - 1], send_sem=send_sem.at[away - 1],
                recv_sem=recv_sem.at[away - 1], device_id={axis: lax.rem(index + away, size)},
                device_id_type=MESH,
            ))
            copies[-1].start()
        return copies

    def gained(copies, source, landing):
        for copy in copies:
            copy.wait()
        value = source[...]
        for away in range(len(copies)):
            value = value + landing[away]
        return value

    def finish(q):
        there = slice(q * columns, (q + 1) * columns)

        def some(step, sums):
            here = pl.ds(pl.multiple_of(step * 512, 512), 512)
            if q == 0:
                extra[here, :] = (total[here, :] * (1.0 / fanout)).astype(BF16)
            value = pre[here, there] + dot(extra[here, :], neigh_w[:, there])
            pre[here, there] = value
            return (
                sums[0] + jnp.sum(value, axis=0, keepdims=True),
                sums[1] + jnp.sum(value * value, axis=0, keepdims=True),
            )

        zero = jnp.zeros((1, columns), F32)
        first, second = lax.fori_loop(0, slots // 512, some, (zero, zero))
        stat_own[q] = jnp.concatenate([first, second, centre[:, there], zero], axis=0)
        near_copies[q] = swap(
            stat_own.at[q], stat_near.at[q], "dev", lane, within, send_near.at[q], recv_near.at[q]
        )

    def relay(q):
        stat_part[q] = gained(near_copies[q], stat_own.at[q], stat_near.at[q])
        far_copies[q] = swap(stat_part.at[q], stat_far.at[q], "hst", host, hosts, send_far.at[q], recv_far.at[q])

    settled = {}

    def settle(q):
        there = slice(q * columns, (q + 1) * columns)
        sums = gained(far_copies[q], stat_part.at[q], stat_far.at[q])
        mean = sums[0:1, :] / total_rows
        variance = sums[1:2, :] / total_rows - mean * mean
        scale = lax.rsqrt(variance + epsilon) * gain_ref[:, there]
        shift = shift_ref[:, there]
        settled[q] = mean, scale, shift
        first_block = q * columns // chunk

        def normal(step, carry):
            here = pl.ds(pl.multiple_of(step * 256, 256), 256)
            hidden = jnp.maximum((pre[here, there] - mean) * scale + shift, 0.0).astype(BF16)
            for c in range(columns // chunk):
                counts[first_block + c, here, :] = hidden[:, c * chunk : (c + 1) * chunk]
            return carry

        lax.fori_loop(0, slots // 256, normal, 0)
        for c in range(columns // chunk):
            both = dot(last_counts[:, 0:slots], counts[first_block + c])
            total[q * targets : (q + 1) * targets, c * chunk : (c + 1) * chunk] = both[0:targets, :]
            at_column = q * columns + c * chunk
            value = dot_nt(self2_ref[:, at_column : at_column + chunk], both[targets:, :].astype(BF16))
            if at_column == 0:
                out_ref[...] = value
            else:
                out_ref[...] += value

    for q in range(shares):
        finish(q)
    for peer in far_peers[half // 2 :]:
        edge_copy(peer).start()
    for q in range(shares - 1):
        relay(q)
    settle(0)
    relay(shares - 1)
    for q in range(1, shares):
        settle(q)

    for away in range(1, within):
        edge_copy(lax.rem(lane + away, within)).wait()
    for q in range(shares):
        there = slice(q * columns, (q + 1) * columns)
        mean, scale, shift = settled[q]
        for away in range(within):
            place = part_of(lax.rem(lane - away + within, within))
            origin = centre[:, there] if away == 0 else stat_near[q, away - 1, 2:3, :]
            value = edge_in[place, there].astype(F32) + (origin - mean)
            edge_in[place, there] = jnp.maximum(value * scale + shift, 0.0).astype(BF16)
        near = total[q * targets : (q + 1) * targets, 0:columns]
        near = near + dot(last_counts[0:targets, slots:], edge_in[:, there])
        out_ref[...] += dot_nt(neigh2_ref[:, there], (near * (1.0 / fanout2)).astype(BF16))

    def drain(away, carry):
        row_copy(lax.rem(me + away, devices)).wait_send()
        return carry

    lax.fori_loop(1, devices, drain, 0)


def local(hot_rows, cold_rows, hot_mask, hot_id, cold_owner, cold_pos, cold_send, adjacency_one, adjacency_two,
          halo_send, self_first, neigh_first, bn_gain, bn_shift, self_second, neigh_second):
    hosts, within = lax.axis_size("hst"), lax.axis_size("dev")
    devices = hosts * within
    nodes, fanout = adjacency_one.shape
    targets, fanout2 = adjacency_two.shape
    slots, edge = cold_send.shape[1], halo_send.shape[1]
    width, units = self_first.shape
    classes = self_second.shape[1]
    assert slots == nodes
    chunk = slots // devices * (within // 2)
    chunks = slots // chunk
    lines = -(-(max(fanout, fanout2) + 1) // 8) * 8
    tiles = slots // LANES
    any_space, vmem = pl.BlockSpec(memory_space=pltpu.HBM), pl.BlockSpec(memory_space=pltpu.VMEM)
    dma = pltpu.SemaphoreType.DMA
    buffers = [pltpu.VMEM((1, nodes), I32) for _ in range(4)] + [
        pltpu.VMEM((1, slots), I32),
        pltpu.VMEM((fanout, nodes), I32),
        pltpu.VMEM((fanout2, targets), I32),
        pltpu.VMEM((1, edge), I32),
        pltpu.VMEM((1, units), F32),
        pltpu.VMEM((1, units), F32),
        pltpu.VMEM((classes, units), BF16),
        pltpu.VMEM((classes, units), BF16),
        pltpu.VMEM(cold_rows.shape, BF16),
        pltpu.VMEM((slots, width), BF16),
        pltpu.VMEM((slots, width), BF16),
        pltpu.VMEM(hot_rows.shape, BF16),
        pltpu.VMEM((slots, width), BF16),
        pltpu.VMEM((chunks, slots, chunk), BF16),
        pltpu.VMEM((chunks, 2 * edge, chunk), BF16),
        pltpu.VMEM((slots, width), F32),
        pltpu.VMEM((2 * edge, width), F32),
        pltpu.VMEM((slots, units), F32),
        pltpu.VMEM((2 * targets, slots + edge), BF16),
        pltpu.VMEM((width, units), BF16),
        pltpu.VMEM((width, units), BF16),
        pltpu.VMEM((edge, units), BF16),
        pltpu.VMEM((edge, units), BF16),
        pltpu.VMEM((slots, LANES), I32),
        pltpu.VMEM((lines, slots), I32),
        pltpu.VMEM((lines, slots), I32),
        pltpu.VMEM((lines, targets), I32),
        pltpu.VMEM((8, slots), I32),
        pltpu.VMEM((2, tiles, LANES), I32),
        pltpu.VMEM((lines, LANES), I32),
        pltpu.VMEM((-(-(tiles + edge // LANES) // 8), lines, LANES), I32),
        pltpu.VMEM((chunk, width), BF16),
        pltpu.VMEM((SHARES, 4, units // SHARES), F32),
        pltpu.VMEM((SHARES, within - 1, 4, units // SHARES), F32),
        pltpu.VMEM((SHARES, 4, units // SHARES), F32),
        pltpu.VMEM((SHARES, hosts - 1, 4, units // SHARES), F32),
    ]
    held = sum(math.prod(b.shape) * b.dtype.itemsize for b in buffers)
    out = pl.pallas_call(
        functools.partial(program, (hosts, within, fanout, fanout2, nodes * devices)),
        in_specs=[any_space] * 16,
        out_specs=vmem,
        out_shape=jax.ShapeDtypeStruct((classes, targets), F32),
        scratch_shapes=buffers + [
            dma((16,)),
            dma((devices,)),
            dma((devices,)),
            dma((within,)),
            dma((within,)),
            dma((SHARES, within - 1)),
            dma((SHARES, within - 1)),
            dma((SHARES, hosts - 1)),
            dma((SHARES, hosts - 1)),
        ],
        compiler_params=pltpu.CompilerParams(
            collective_id=0, has_side_effects=True, vmem_limit_bytes=min(held + 9 * MIB, 63 * MIB)
        ),
        name="sage",
    )(
        hot_rows, cold_rows, hot_mask[None, :], hot_id[None, :], cold_owner[None, :], cold_pos[None, :], cold_send,
        adjacency_one.T, adjacency_two.T, halo_send, self_first, neigh_first, bn_gain[None, :], bn_shift[None, :],
        self_second.T, neigh_second.T,
    )
    return out.T


def solution(mesh):
    owned, split, copied = P(("hst", "dev"), None), P(("hst", "dev")), P()
    placed = (copied, owned) + (split,) * 4 + (owned,) * 4 + (copied,) * 6
    return jax.shard_map(local, mesh=mesh, in_specs=placed, out_specs=owned, check_vma=False)
```
